32 devices in a mesh: lat: 4 (over z), lon: 4 (over y, x), obs: 2 (over core).
Axes of the slice: x: 2, y: 2, z: 4, core: 2. Of those that a mesh axis runs over, the one named last changes fastest.
Arguments:
- innovation: float32 [4096, 128], P(('lat', 'lon', 'obs')), may hold values from -6 to 6
- obs_error: float32 [4096, 128], P(('lat', 'lon', 'obs')), may hold values from 0.5 to 2
- obs_offset: float32 [2, 4096, 128], P(None, ('lat', 'lon', 'obs')), may hold values from 0 to 1
- obs_cell: int32 [4096, 128], P(('lat', 'lon', 'obs')), may hold values from 0 to 65535
- obs_owner: int32 [32, 128], P(('lat', 'lon', 'obs')), may hold values from 0 to 15, as said below
- block_count: int32 [32], P(('lat', 'lon', 'obs')), may hold values from 64 to 128
- land_mask: int32 [256, 4096], P(('lat', 'obs'), 'lon'), may hold values from 0 to 1, as said below
- inertia: float32 [256, 4096], P(('lat', 'obs'), 'lon'), may hold values from 0.002 to 0.05
- sea_depth: float32 [256, 4096], P(('lat', 'obs'), 'lon'), may hold values from 0.5 to 5
Outputs:
- adjoint_field: float32 [256, 4096], P(('lat', 'obs'), 'lon')
- residual: float32 [256, 4096], P(('lat', 'obs'), 'lon')
The draws below stay inside these ranges and needn't reach their ends.
Inputs may be any that keep to these rules, and one draw needn't show every extreme that they name: `obs_owner`: among the live blocks of one device at most 16 name the same tile; in every draw some tile is named by exactly 16 live blocks of every device. `land_mask`: the first and the last grid row are land.
All inputs are finite; a program needn't handle non-finite values.
Results may differ from the reference program's by a relative error of at most 0.0003.
Values sent between devices are 32-bit elements; how exact they have to be, the bound alone decides.
A program may use at most 64 MiB of HBM per device.

```python
import math
import jax
import jax.numpy as jnp

TILE_R = 64
TILE_C = 1024
NBLK = 128
BLOCK = 128
ITERS = 5
CAPB = 16
NLAT = 256
NLON = 4096
N_LAT = 4
N_LON = 4
DEVICES = 32


def owner_plan(key):
    tile_count = N_LAT * N_LON
    slot_total = tile_count * CAPB
    base_key = jax.random.fold_in(key, 7711)
    block_counts = jax.random.randint(jax.random.fold_in(base_key, 1), (DEVICES,), NBLK // 2, NBLK + 1)
    hot_tile = jax.random.randint(jax.random.fold_in(base_key, 2), (), 0, tile_count)
    device_keys = jax.random.split(jax.random.fold_in(base_key, 3), DEVICES)

    def device_plan(dev_key, live_total):
        perm_key, mix_key = jax.random.split(dev_key)
        shuffled = jax.random.permutation(perm_key, slot_total)
        slot_ids = jnp.arange(slot_total)
        is_hot = slot_ids // CAPB == hot_tile
        sort_key = jnp.where(is_hot, slot_ids - slot_total, shuffled)
        chosen = jnp.argsort(sort_key)[:NBLK]
        owners = chosen // CAPB
        block_ids = jnp.arange(NBLK)
        mixing = jax.random.permutation(mix_key, NBLK)
        live_key = jnp.where(block_ids < live_total, mixing, NBLK + block_ids)
        return owners[jnp.argsort(live_key)]
    owners = jax.vmap(device_plan)(device_keys, block_counts)
    return (block_counts.astype(jnp.int32), owners.astype(jnp.int32))


def draw_obs_owner(key, part):
    return owner_plan(key)[1]


def draw_block_count(key, part):
    return owner_plan(key)[0]


def draw_land_mask(key, part):
    land_bits = jax.random.randint(jax.random.fold_in(key, 913), (NLAT, NLON), 0, 10)
    row_ids = jnp.arange(NLAT)[:, None]
    ocean = (land_bits < 7) & (row_ids > 0) & (row_ids < NLAT - 1)
    return ocean.astype(jnp.int32)


def touch_ends(result, rng, smallest, top_value):
    shape = result.shape
    index_at = [jax.random.randint(jax.random.fold_in(rng, axis), (), 0, shape[axis]) for axis in range(len(shape))]
    result = result.at[tuple(index_at)].set(smallest)
    longest = shape.index(max(shape))
    index_at[longest] = (index_at[longest] + 1) % shape[longest]
    return result.at[tuple(index_at)].set(top_value)


def block_levels(own_key, extent, cuts, smallest, high):
    level, own = 1.0, jax.random.fold_in(own_key, 6)
    for axis_at, blocks in cuts:
        steps = jnp.exp(jax.random.uniform(jax.random.fold_in(own, axis_at), (blocks,), jnp.float32, smallest / len(cuts), high / len(cuts)))
        level = level * jnp.repeat(steps, extent[axis_at] // blocks).reshape([-1 if axis == axis_at else 1 for axis in range(len(extent))])
    return level


def bell_draw(key, shape, deviation, limit, cuts=(), held_as=jnp.bfloat16):
    gain = block_levels(key, shape, cuts, -0.22, 0.18) if cuts else 1.0
    array = jax.random.normal(key, shape, jnp.float32) * deviation * gain
    return jnp.minimum(jnp.maximum(array, -limit), limit).astype(held_as)


def setup_inputs(seed: int = 0) -> dict:
    splits = jax.random.split(jax.random.key(seed), 10)
    return {
        "innovation": bell_draw(splits[0], (DEVICES * NBLK, BLOCK), 1.0, 6.0, ((0, 32),), jnp.float32),
        "obs_error": jnp.clip(jnp.exp(math.log(2.0) - 1.3862944 * jax.random.uniform(splits[1], (DEVICES * NBLK, BLOCK), jnp.float32) ** block_levels(splits[1], (DEVICES * NBLK, BLOCK), ((0, 32),), -0.2, 0.2)), 0.5, 2.0),
        "obs_offset": jnp.clip(1.0 * jax.random.uniform(splits[2], (2, DEVICES * NBLK, BLOCK), jnp.float32) ** block_levels(splits[2], (2, DEVICES * NBLK, BLOCK), ((1, 32),), -0.2, 0.2), 0.0, 1.0),
        "obs_cell": touch_ends(jax.random.randint(splits[3], (DEVICES * NBLK, BLOCK), 0, TILE_R * TILE_C), jax.random.fold_in(splits[3], 1), 0, (TILE_R * TILE_C) - 1).astype(jnp.int32),
        "obs_owner": draw_obs_owner(jax.random.fold_in(splits[9], 71), 0),
        "block_count": draw_block_count(jax.random.fold_in(splits[9], 71), 0),
        "land_mask": draw_land_mask(jax.random.fold_in(splits[9], 71), 0),
        "inertia": jnp.clip(jnp.exp(math.log(0.05) - 3.218876 * jax.random.uniform(splits[7], (NLAT, NLON), jnp.float32) ** block_levels(splits[7], (NLAT, NLON), ((0, 8), (1, 4)), -0.2, 0.2)), 0.002, 0.05),
        "sea_depth": jnp.clip(jnp.exp(math.log(5.0) - 2.3025851 * jax.random.uniform(splits[8], (NLAT, NLON), jnp.float32) ** block_levels(splits[8], (NLAT, NLON), ((0, 8), (1, 4)), -0.2, 0.2)), 0.5, 5.0),
    }


def reference(innovation, obs_error, obs_offset, obs_cell, obs_owner, block_count, land_mask, inertia, sea_depth):
    is_live = (jnp.arange(NBLK)[None, :] < block_count[:, None]).reshape(-1)
    owner_tile = obs_owner.reshape(-1)
    scaled = jnp.where(is_live[:, None], innovation / (obs_error * obs_error), jnp.float32(0.0))
    north_frac = obs_offset[0]
    east_frac = obs_offset[1]
    cell_row = (owner_tile // N_LON)[:, None] * TILE_R + obs_cell // TILE_C
    cell_col = (owner_tile % N_LON)[:, None] * TILE_C + obs_cell % TILE_C
    next_col = (cell_col + 1) % NLON
    next_row = cell_row + 1
    cell_total = NLAT * NLON
    inside = next_row < NLAT
    segment_ids = jnp.concatenate([(cell_row * NLON + cell_col).reshape(-1), (cell_row * NLON + next_col).reshape(-1), jnp.where(inside, next_row * NLON + cell_col, cell_total).reshape(-1), jnp.where(inside, next_row * NLON + next_col, cell_total).reshape(-1)]).astype(jnp.int32)
    contribs = jnp.concatenate([(scaled * ((1.0 - north_frac) * (1.0 - east_frac))).reshape(-1), (scaled * ((1.0 - north_frac) * east_frac)).reshape(-1), (scaled * (north_frac * (1.0 - east_frac))).reshape(-1), (scaled * (north_frac * east_frac)).reshape(-1)])
    partial_value = jax.ops.segment_sum(contribs, segment_ids, num_segments=cell_total + 1)[:cell_total]
    ocean = land_mask.astype(jnp.float32)
    forcing = partial_value.reshape(NLAT, NLON) * ocean
    conduct = ocean * sea_depth
    cond_north = jnp.sqrt(conduct * jnp.roll(conduct, 1, 0))
    cond_south = jnp.sqrt(conduct * jnp.roll(conduct, -1, 0))
    cond_west = jnp.sqrt(conduct * jnp.roll(conduct, 1, 1))
    cond_east = jnp.sqrt(conduct * jnp.roll(conduct, -1, 1))
    diagonal = inertia + cond_north + cond_south + cond_west + cond_east

    def operate(field):
        return diagonal * field - cond_north * jnp.roll(field, 1, 0) - cond_south * jnp.roll(field, -1, 0) - cond_west * jnp.roll(field, 1, 1) - cond_east * jnp.roll(field, -1, 1)
    adjoint_field = jnp.zeros_like(forcing)
    residual = forcing
    direction = forcing
    norm_now = jnp.sum(residual * residual)
    for iteration in range(ITERS):
        applied = operate(direction)
        step_size = norm_now / jnp.sum(direction * applied)
        adjoint_field = adjoint_field + step_size * direction
        residual = residual - step_size * applied
        norm_next = jnp.sum(residual * residual)
        direction = residual + norm_next / norm_now * direction
        norm_now = norm_next
    return (adjoint_field, residual)
```

```python
import functools

import jax
import jax.numpy as jnp
from jax import lax
from jax.experimental import pallas as pl
from jax.experimental.pallas import tpu as pltpu
from jax.sharding import PartitionSpec as P

ITERS = 5
ROW_PAD = 8
COL_PAD = 128
MESH = pl.DeviceIdType.MESH
AXES = ("lat", "lon", "obs")


def spread_kernel(row_span, half, d_ref, out_ref, acc_ref):
    step = pl.program_id(0)
    rows_all = 2 * row_span
    amount = d_ref[0, 0]
    north = d_ref[0, 1]
    east = d_ref[0, 2]
    key = d_ref[0, 3]
    row_id = jnp.floor(key * (1.0 / half))
    col_id = key - row_id * half - (half // 2)
    upper = amount * (1.0 - north)
    lower = amount * north
    pairs = []
    for share in (1.0 - east, east):
        top, bottom = upper * share, lower * share
        top_high = top.astype(jnp.bfloat16).astype(jnp.float32)
        bottom_high = bottom.astype(jnp.bfloat16).astype(jnp.float32)
        pairs.append((top_high, bottom_high))
        pairs.append((top - top_high, bottom - bottom_high))

    def wide(values, slot, count):
        tile = jnp.broadcast_to(values[slot : slot + 1], (16, values.shape[1]))
        tile = tile.astype(jnp.bfloat16)
        return jnp.concatenate([tile] * (count // 16), axis=0)

    width = amount.shape[1]
    row_axis = lax.broadcasted_iota(jnp.int32, (rows_all, width), 0)
    row_axis = row_axis.astype(jnp.float32).astype(jnp.bfloat16)
    row_axis_low = lax.broadcasted_iota(jnp.int32, (rows_all, width), 0) - 1
    row_axis_low = row_axis_low.astype(jnp.float32).astype(jnp.bfloat16)
    col_axis = lax.broadcasted_iota(jnp.int32, (half, width), 0) - (half // 2)
    col_axis = col_axis.astype(jnp.float32).astype(jnp.bfloat16)
    zero = jnp.zeros((), jnp.bfloat16)
    one = jnp.ones((), jnp.bfloat16)
    left, right = [], []
    for slot in range(amount.shape[0]):
        ids = wide(row_id, slot, rows_all)
        is_top = row_axis == ids
        is_bottom = row_axis_low == ids
        planes = [
            jnp.where(
                is_top,
                wide(top, slot, rows_all),
                jnp.where(is_bottom, wide(bottom, slot, rows_all), zero),
            )
            for top, bottom in pairs
        ]
        left.append(jnp.concatenate(planes, axis=0))
        right.append(jnp.where(col_axis == wide(col_id, slot, half), one, zero))
    product = lax.dot_general(
        jnp.concatenate(left, axis=1),
        jnp.concatenate(right, axis=1),
        (((1,), (1,)), ((), ())),
        preferred_element_type=jnp.float32,
    )

    @pl.when(step == 0)
    def _():
        acc_ref[...] = product

    @pl.when(step > 0)
    def _():
        acc_ref[...] = acc_ref[...] + product

    @pl.when(step == pl.num_programs(0) - 1)
    def _():
        def plane(index):
            first = acc_ref[2 * index * rows_all : (2 * index + 1) * rows_all]
            first = first + acc_ref[(2 * index + 1) * rows_all : (2 * index + 2) * rows_all]
            return jnp.concatenate([first[:row_span], first[row_span:]], axis=1)

        moved = pltpu.roll(plane(1), 1, 1)
        col = lax.broadcasted_iota(jnp.int32, moved.shape, 1)
        out_ref[:, : 2 * half] = plane(0) + jnp.where(col > 0, moved, 0.0)
        out_ref[:, 2 * half :] = jnp.where(
            col[:, :COL_PAD] == 0, moved[:, :COL_PAD], 0.0
        )


def solve_kernel(
    t_ref, g_ref, x_ref, r_ref,
    pair_ref, win_ref, west_ref, east_ref, edge_ref, wide_ref,
    up_ref, down_ref, mid_ref, cwest_ref, ceast_ref,
    diag_ref, cn_ref, cs_ref, cw_ref, ce_ref, res_ref, app_ref, dir_ref, adir_ref, sol_ref,
    part_ref, slot_ref, send_sem, recv_sem, sum_send, sum_recv,
):
    n_lat, n_lon, n_obs = (lax.axis_size(name) for name in AXES)
    lat, lon, core = (lax.axis_index(name) for name in AXES)
    total = n_lat * n_lon * n_obs
    me = (lat * n_lon + lon) * n_obs + core
    rows, cols = x_ref.shape
    tall = rows + 2 * ROW_PAD
    keep = rows + ROW_PAD

    def place(flat):
        return (flat // (n_lon * n_obs), (flat // n_obs) % n_lon, flat % n_obs)

    barrier = pltpu.get_barrier_semaphore()

    def greet(k, carry):
        pl.semaphore_signal(
            barrier, inc=1, device_id=place(lax.rem(me + k, total)), device_id_type=MESH
        )
        return carry

    lax.fori_loop(1, total, greet, 0)
    pl.semaphore_wait(barrier, total - 1)

    def copy(index, source, target, device):
        return pltpu.make_async_remote_copy(
            src_ref=source,
            dst_ref=target,
            send_sem=send_sem.at[index],
            recv_sem=recv_sem.at[index],
            device_id=device,
            device_id_type=MESH,
        )

    ring = n_lat * n_obs
    line = lat * n_obs + core
    above = lax.rem(line + ring - 1, ring)
    below = lax.rem(line + 1, ring)
    west = lax.rem(lon + n_lon - 1, n_lon)
    east = lax.rem(lon + 1, n_lon)
    split = rows - ROW_PAD
    mine = pl.multiple_of(core * split, 8)
    theirs = pl.multiple_of((1 - core) * split, 8)
    swap = copy(0, t_ref.at[pl.ds(theirs, tall)], pair_ref, (lat, lon, 1 - core))
    to_below = copy(
        1, g_ref.at[:, pl.ds(rows - ROW_PAD, ROW_PAD)], up_ref, (below // n_obs, lon, below % n_obs)
    )
    to_above = copy(
        2, g_ref.at[:, pl.ds(0, ROW_PAD)], down_ref, (above // n_obs, lon, above % n_obs)
    )
    swap.start()
    to_below.start()
    to_above.start()
    to_below.wait()
    to_above.wait()
    mid_ref[:, :ROW_PAD] = up_ref[...]
    mid_ref[:, ROW_PAD:keep] = g_ref[...]
    mid_ref[:, keep:] = down_ref[...]
    c_east = copy(3, mid_ref.at[:, :, pl.ds(cols - COL_PAD, COL_PAD)], cwest_ref, (lat, east, core))
    c_west = copy(4, mid_ref.at[:, :, pl.ds(0, COL_PAD)], ceast_ref, (lat, west, core))
    c_east.start()
    c_west.start()
    swap.wait()
    win_ref[...] = t_ref[pl.ds(mine, tall)] + pair_ref[...]
    t_east = copy(
        5, win_ref.at[:, pl.ds(cols - COL_PAD, 2 * COL_PAD)], west_ref, (lat, east, core)
    )
    t_west = copy(6, win_ref.at[:, pl.ds(0, COL_PAD)], east_ref, (lat, west, core))
    t_east.start()
    t_west.start()
    t_east.wait()
    t_west.wait()
    wide_ref[:, :COL_PAD] = west_ref[:, :COL_PAD]
    wide_ref[:, COL_PAD : 2 * COL_PAD] = win_ref[:, :COL_PAD] + west_ref[:, COL_PAD:]
    wide_ref[:, 2 * COL_PAD : COL_PAD + cols] = win_ref[:, COL_PAD:cols]
    wide_ref[:, COL_PAD + cols :] = east_ref[...] + win_ref[:, cols:]
    side = lax.rem(lat + n_lat + 2 * core - 1, n_lat)
    t_rows = copy(
        7,
        wide_ref.at[pl.ds(pl.multiple_of(core * rows, 8), 2 * ROW_PAD)],
        edge_ref,
        (side, lon, 1 - core),
    )
    t_rows.start()
    c_east.wait()
    c_west.wait()

    def widened(index):
        return jnp.concatenate([cwest_ref[index], mid_ref[index], ceast_ref[index]], axis=1)

    def moved(value, axis, back):
        size = value.shape[axis]
        return pltpu.roll(value, size - 1 if back else 1, axis)

    conduct = widened(0)
    cn = jnp.sqrt(conduct * moved(conduct, 0, False))
    cs = jnp.sqrt(conduct * moved(conduct, 0, True))
    cw = jnp.sqrt(conduct * moved(conduct, 1, False))
    ce = jnp.sqrt(conduct * moved(conduct, 1, True))
    cn_ref[...] = cn
    cs_ref[...] = cs
    cw_ref[...] = cw
    ce_ref[...] = ce
    diag_ref[...] = widened(1) + cn + cs + cw + ce
    t_rows.wait()

    @pl.when(core == 0)
    def _():
        spill = jnp.where(lat > 0, 1.0, 0.0)
        res_ref[:ROW_PAD] = edge_ref[:ROW_PAD]
        res_ref[ROW_PAD : 2 * ROW_PAD] = wide_ref[:ROW_PAD] + edge_ref[ROW_PAD:] * spill
        res_ref[2 * ROW_PAD :] = wide_ref[ROW_PAD:keep]

    @pl.when(core == 1)
    def _():
        spill = jnp.where(lat < n_lat - 1, 1.0, 0.0)
        res_ref[:keep] = wide_ref[:keep]
        res_ref[keep:] = edge_ref[:ROW_PAD] + wide_ref[keep:] * spill

    ocean = jnp.where(widened(0) > 0.0, 1.0, 0.0)
    res_ref[...] = res_ref[...] * ocean

    def inner(value):
        return value[ROW_PAD:keep, COL_PAD : COL_PAD + cols]

    def fold(value):
        value = inner(value)
        out = value[:8]
        for start in range(8, rows, 8):
            out = out + value[start : start + 8]
        lanes = out[:, :COL_PAD]
        for start in range(COL_PAD, cols, COL_PAD):
            lanes = lanes + out[:, start : start + COL_PAD]
        return jnp.sum(lanes, axis=(0, 1), keepdims=True)

    lane = lax.broadcasted_iota(jnp.int32, (1, COL_PAD), 1)

    def operate():
        field = res_ref[...]
        applied = (
            diag_ref[...] * field
            - cn_ref[...] * moved(field, 0, False)
            - cs_ref[...] * moved(field, 0, True)
            - cw_ref[...] * moved(field, 1, False)
            - ce_ref[...] * moved(field, 1, True)
        )
        app_ref[...] = applied
        first, second = fold(field * field), fold(field * applied)
        return jnp.where(lane == 0, first, jnp.where(lane == 1, second, 0.0))

    def reduced(values, turn):
        slot_ref[turn, pl.ds(me, 1)] = values[None]
        part_ref[turn] = values

        def post(k, carry):
            pltpu.make_async_remote_copy(
                src_ref=part_ref.at[turn],
                dst_ref=slot_ref.at[turn, me],
                send_sem=sum_send.at[turn],
                recv_sem=sum_recv.at[turn],
                device_id=place(lax.rem(me + k, total)),
                device_id_type=MESH,
            ).start()
            return carry

        lax.fori_loop(1, total, post, 0)
        block = slot_ref.at[turn, pl.ds(0, total - 1)]
        pltpu.make_async_copy(block, block, sum_recv.at[turn]).wait()
        pltpu.make_async_copy(block, block, sum_send.at[turn]).wait()
        sums = jnp.sum(slot_ref[turn], axis=0)
        return sums[:, 0:1], sums[:, 1:2]

    norm_now, product = reduced(operate(), 0)
    step_size = norm_now / product
    dir_ref[...] = res_ref[...]
    adir_ref[...] = app_ref[...]
    for turn in range(ITERS):
        scaled = step_size * inner(dir_ref[...])
        sol_ref[...] = scaled if turn == 0 else sol_ref[...] + scaled
        res_ref[...] = res_ref[...] - step_size * adir_ref[...]
        if turn + 1 < ITERS:
            norm_next, product = reduced(operate(), turn + 1)
            ratio = norm_next / norm_now
            step_size = norm_next / (product - ratio * norm_next / step_size)
            dir_ref[...] = res_ref[...] + ratio * dir_ref[...]
            adir_ref[...] = app_ref[...] + ratio * adir_ref[...]
            norm_now = norm_next
    x_ref[...] = sol_ref[...]
    r_ref[...] = inner(res_ref[...])


def body(
    innovation, obs_error, obs_offset, obs_cell, obs_owner, block_count,
    land_mask, inertia, sea_depth,
):
    block_total = obs_owner.shape[1]
    block_width = innovation.shape[1]
    n_lat, n_lon, n_obs = (lax.axis_size(name) for name in AXES)
    tile_count = n_lat * n_lon
    capacity = max(3, 2 * ((block_total + tile_count - 1) // tile_count))
    rows, cols = land_mask.shape
    tile_rows = rows * n_obs
    half = cols // 2
    row_span = tile_rows + 8
    total = tile_count * n_obs
    owners = obs_owner[0]
    block_ids = jnp.arange(block_total)
    is_live = block_ids < block_count[0]
    earlier = block_ids[None, :] < block_ids[:, None]
    same_owner = (owners[None, :] == owners[:, None]) & earlier & is_live[None, :]
    slot_rank = jnp.sum(same_owner.astype(jnp.int32), axis=1)
    target = jnp.where(is_live, owners * capacity + slot_rank, tile_count * capacity)
    place = (jnp.arange(tile_count * capacity)[:, None] == target[None, :]).astype(jnp.float32)
    scaled = innovation / (obs_error * obs_error)
    cell_row, cell_col = obs_cell // cols, obs_cell % cols
    key = ((cell_col // half) * row_span + cell_row) * half + cell_col % half
    data = jnp.stack([scaled, obs_offset[0], obs_offset[1], key.astype(jnp.float32)], axis=1)
    sent = jnp.dot(
        place,
        data.reshape(block_total, 4 * block_width),
        precision=lax.Precision.HIGHEST,
        preferred_element_type=jnp.float32,
    )
    sent = sent.reshape(tile_count, capacity, 4, block_width).transpose(0, 2, 1, 3)
    received = lax.all_to_all(sent, ("lat", "lon"), split_axis=0, concat_axis=0, tiled=True)
    tile = pl.pallas_call(
        functools.partial(spread_kernel, row_span, half),
        grid=(tile_count,),
        in_specs=[pl.BlockSpec((1, 4, capacity, block_width), lambda i: (i, 0, 0, 0))],
        out_specs=pl.BlockSpec((row_span, cols + COL_PAD), lambda i: (0, 0)),
        out_shape=jax.ShapeDtypeStruct((row_span, cols + COL_PAD), jnp.float32),
        scratch_shapes=[pltpu.VMEM((8 * row_span, half), jnp.float32)],
        compiler_params=pltpu.CompilerParams(dimension_semantics=("arbitrary",)),
        name="spread",
    )(received)
    conduct = land_mask.astype(jnp.float32) * sea_depth
    ground = jnp.stack([conduct, inertia])
    tall, broad = rows + 2 * ROW_PAD, cols + 2 * COL_PAD
    vmem = lambda *shape: pltpu.VMEM(shape, jnp.float32)
    return pl.pallas_call(
        solve_kernel,
        out_shape=[jax.ShapeDtypeStruct((rows, cols), jnp.float32)] * 2,
        in_specs=[pl.BlockSpec(memory_space=pltpu.VMEM)] * 2,
        out_specs=[pl.BlockSpec(memory_space=pltpu.VMEM)] * 2,
        scratch_shapes=[
            vmem(tall, cols + COL_PAD),
            vmem(tall, cols + COL_PAD),
            vmem(tall, 2 * COL_PAD),
            vmem(tall, COL_PAD),
            vmem(2 * ROW_PAD, broad),
            vmem(tall, broad),
            vmem(2, ROW_PAD, cols),
            vmem(2, ROW_PAD, cols),
            vmem(2, tall, cols),
            vmem(2, tall, COL_PAD),
            vmem(2, tall, COL_PAD),
        ]
        + [vmem(tall, broad)] * 9
        + [
            vmem(rows, cols),
            vmem(ITERS, 1, COL_PAD),
            vmem(ITERS, total, 1, COL_PAD),
            pltpu.SemaphoreType.DMA((8,)),
            pltpu.SemaphoreType.DMA((8,)),
            pltpu.SemaphoreType.DMA((ITERS,)),
            pltpu.SemaphoreType.DMA((ITERS,)),
        ],
        compiler_params=pltpu.CompilerParams(collective_id=0, has_side_effects=True),
        name="solve",
    )(tile, ground)


def solution(mesh):
    spread = P(AXES, None)
    grid = P(("lat", "obs"), "lon")
    in_specs = (spread, spread, P(None, AXES, None), spread, spread, P(AXES), grid, grid, grid)
    return jax.shard_map(
        body, mesh=mesh, in_specs=in_specs, out_specs=(grid, grid), check_vma=False
    )
```

```python
import functools

import jax
import jax.numpy as jnp
from jax import lax
from jax.experimental import pallas as pl
from jax.experimental.pallas import tpu as pltpu
from jax.sharding import PartitionSpec as P

ITERS = 5
STAGES = (2, 2, 1)
ROW_PAD = 8
COL_PAD = 128
MESH = pl.DeviceIdType.MESH
AXES = ("lat", "lon", "obs")


def spread_kernel(row_span, half, d_ref, out_ref, inbox_ref, acc_ref, send_sem, recv_sem):
    n_lon = lax.axis_size("lon")
    count = lax.axis_size("lat") * n_lon
    core = lax.axis_index("obs")
    me = lax.axis_index("lat") * n_lon + lax.axis_index("lon")
    barrier = pltpu.get_barrier_semaphore()

    def place(flat):
        return (flat // n_lon, flat % n_lon, core)

    def greet(k, carry):
        pl.semaphore_signal(
            barrier, inc=1, device_id=place(lax.rem(me + k, count)), device_id_type=MESH
        )
        return carry

    def copy(k):
        target = lax.rem(me + k, count)
        return pltpu.make_async_remote_copy(
            src_ref=d_ref.at[target],
            dst_ref=inbox_ref.at[k],
            send_sem=send_sem.at[k],
            recv_sem=recv_sem.at[k],
            device_id=place(target),
            device_id_type=MESH,
        )

    def send(k, carry):
        copy(k).start()
        return carry

    def finish(k, carry):
        copy(k).wait_send()
        return carry

    lax.fori_loop(1, count, greet, 0)
    pl.semaphore_wait(barrier, count - 1)
    lax.fori_loop(1, count, send, 0)
    acc_ref[...] = spread_block(row_span, half, d_ref[me])

    def turn(k, carry):
        copy(k).wait_recv()
        acc_ref[...] = acc_ref[...] + spread_block(row_span, half, inbox_ref[k])
        return carry

    lax.fori_loop(1, count, turn, 0)
    lax.fori_loop(1, count, finish, 0)
    rows_all = 2 * row_span

    def plane(index):
        first = acc_ref[2 * index * rows_all : (2 * index + 1) * rows_all]
        first = first + acc_ref[(2 * index + 1) * rows_all : (2 * index + 2) * rows_all]
        return jnp.concatenate([first[:row_span], first[row_span:]], axis=1)

    moved = pltpu.roll(plane(1), 1, 1)
    col = lax.broadcasted_iota(jnp.int32, moved.shape, 1)
    out_ref[:, : 2 * half] = plane(0) + jnp.where(col > 0, moved, 0.0)
    out_ref[:, 2 * half :] = jnp.where(col[:, :COL_PAD] == 0, moved[:, :COL_PAD], 0.0)


def spread_block(row_span, half, block):
    rows_all = 2 * row_span
    amount = block[0]
    north = block[1]
    east = block[2]
    key = block[3]
    row_id = jnp.floor(key * (1.0 / half))
    col_id = key - row_id * half - (half // 2)
    upper = amount * (1.0 - north)
    lower = amount * north
    pairs = []
    for share in (1.0 - east, east):
        top, bottom = upper * share, lower * share
        top_high = top.astype(jnp.bfloat16).astype(jnp.float32)
        bottom_high = bottom.astype(jnp.bfloat16).astype(jnp.float32)
        pairs.append((top_high, bottom_high))
        pairs.append((top - top_high, bottom - bottom_high))

    def wide(values, slot, count):
        tile = jnp.broadcast_to(values[slot : slot + 1], (16, values.shape[1]))
        tile = tile.astype(jnp.bfloat16)
        return jnp.concatenate([tile] * (count // 16), axis=0)

    width = amount.shape[1]
    row_axis = lax.broadcasted_iota(jnp.int32, (rows_all, width), 0)
    row_axis = row_axis.astype(jnp.float32).astype(jnp.bfloat16)
    row_axis_low = lax.broadcasted_iota(jnp.int32, (rows_all, width), 0) - 1
    row_axis_low = row_axis_low.astype(jnp.float32).astype(jnp.bfloat16)
    col_axis = lax.broadcasted_iota(jnp.int32, (half, width), 0) - (half // 2)
    col_axis = col_axis.astype(jnp.float32).astype(jnp.bfloat16)
    zero = jnp.zeros((), jnp.bfloat16)
    one = jnp.ones((), jnp.bfloat16)
    left, right = [], []
    for slot in range(amount.shape[0]):
        ids = wide(row_id, slot, rows_all)
        is_top = row_axis == ids
        is_bottom = row_axis_low == ids
        planes = [
            jnp.where(
                is_top,
                wide(top, slot, rows_all),
                jnp.where(is_bottom, wide(bottom, slot, rows_all), zero),
            )
            for top, bottom in pairs
        ]
        left.append(jnp.concatenate(planes, axis=0))
        right.append(jnp.where(col_axis == wide(col_id, slot, half), one, zero))
    return lax.dot_general(
        jnp.concatenate(left, axis=1),
        jnp.concatenate(right, axis=1),
        (((1,), (1,)), ((), ())),
        preferred_element_type=jnp.float32,
    )


def solve_kernel(
    t_ref, g_ref, x_ref, r_ref,
    pair_ref, win_ref, west_ref, east_ref, edge_ref, wide_ref,
    up_ref, down_ref, mid_ref, cwest_ref, ceast_ref,
    diag_ref, cn_ref, cs_ref, cw_ref, ce_ref, res_ref, app_ref, dir_ref, adir_ref, far_ref, sol_ref,
    part_ref, slot_ref, send_sem, recv_sem, sum_send, sum_recv,
):
    n_lat, n_lon, n_obs = (lax.axis_size(name) for name in AXES)
    lat, lon, core = (lax.axis_index(name) for name in AXES)
    total = n_lat * n_lon * n_obs
    me = (lat * n_lon + lon) * n_obs + core
    rows, cols = x_ref.shape
    tall = rows + 2 * ROW_PAD
    keep = rows + ROW_PAD

    def place(flat):
        return (flat // (n_lon * n_obs), (flat // n_obs) % n_lon, flat % n_obs)

    barrier = pltpu.get_barrier_semaphore()

    def greet(k, carry):
        pl.semaphore_signal(
            barrier, inc=1, device_id=place(lax.rem(me + k, total)), device_id_type=MESH
        )
        return carry

    lax.fori_loop(1, total, greet, 0)
    pl.semaphore_wait(barrier, total - 1)

    def copy(index, source, target, device):
        return pltpu.make_async_remote_copy(
            src_ref=source,
            dst_ref=target,
            send_sem=send_sem.at[index],
            recv_sem=recv_sem.at[index],
            device_id=device,
            device_id_type=MESH,
        )

    ring = n_lat * n_obs
    line = lat * n_obs + core
    above = lax.rem(line + ring - 1, ring)
    below = lax.rem(line + 1, ring)
    west = lax.rem(lon + n_lon - 1, n_lon)
    east = lax.rem(lon + 1, n_lon)
    split = rows - ROW_PAD
    mine = pl.multiple_of(core * split, 8)
    theirs = pl.multiple_of((1 - core) * split, 8)
    swap = copy(0, t_ref.at[pl.ds(theirs, tall)], pair_ref, (lat, lon, 1 - core))
    to_below = copy(
        1, g_ref.at[:, pl.ds(rows - ROW_PAD, ROW_PAD)], up_ref, (below // n_obs, lon, below % n_obs)
    )
    to_above = copy(
        2, g_ref.at[:, pl.ds(0, ROW_PAD)], down_ref, (above // n_obs, lon, above % n_obs)
    )
    swap.start()
    to_below.start()
    to_above.start()
    to_below.wait()
    to_above.wait()
    mid_ref[:, :ROW_PAD] = up_ref[...]
    mid_ref[:, ROW_PAD:keep] = g_ref[...]
    mid_ref[:, keep:] = down_ref[...]
    c_east = copy(3, mid_ref.at[:, :, pl.ds(cols - COL_PAD, COL_PAD)], cwest_ref, (lat, east, core))
    c_west = copy(4, mid_ref.at[:, :, pl.ds(0, COL_PAD)], ceast_ref, (lat, west, core))
    c_east.start()
    c_west.start()
    swap.wait()
    win_ref[...] = t_ref[pl.ds(mine, tall)] + pair_ref[...]
    t_east = copy(
        5, win_ref.at[:, pl.ds(cols - COL_PAD, 2 * COL_PAD)], west_ref, (lat, east, core)
    )
    t_west = copy(6, win_ref.at[:, pl.ds(0, COL_PAD)], east_ref, (lat, west, core))
    t_east.start()
    t_west.start()
    t_east.wait()
    t_west.wait()
    wide_ref[:, :COL_PAD] = west_ref[:, :COL_PAD]
    wide_ref[:, COL_PAD : 2 * COL_PAD] = win_ref[:, :COL_PAD] + west_ref[:, COL_PAD:]
    wide_ref[:, 2 * COL_PAD : COL_PAD + cols] = win_ref[:, COL_PAD:cols]
    wide_ref[:, COL_PAD + cols :] = east_ref[...] + win_ref[:, cols:]
    side = lax.rem(lat + n_lat + 2 * core - 1, n_lat)
    t_rows = copy(
        7,
        wide_ref.at[pl.ds(pl.multiple_of(core * rows, 8), 2 * ROW_PAD)],
        edge_ref,
        (side, lon, 1 - core),
    )
    t_rows.start()
    c_east.wait()
    c_west.wait()

    def widened(index):
        return jnp.concatenate([cwest_ref[index], mid_ref[index], ceast_ref[index]], axis=1)

    def moved(value, axis, back):
        size = value.shape[axis]
        return pltpu.roll(value, size - 1 if back else 1, axis)

    conduct = widened(0)
    cn = jnp.sqrt(conduct * moved(conduct, 0, False))
    cs = jnp.sqrt(conduct * moved(conduct, 0, True))
    cw = jnp.sqrt(conduct * moved(conduct, 1, False))
    ce = jnp.sqrt(conduct * moved(conduct, 1, True))
    cn_ref[...] = cn
    cs_ref[...] = cs
    cw_ref[...] = cw
    ce_ref[...] = ce
    diag_ref[...] = widened(1) + cn + cs + cw + ce
    t_rows.wait()

    @pl.when(core == 0)
    def _():
        spill = jnp.where(lat > 0, 1.0, 0.0)
        res_ref[:ROW_PAD] = edge_ref[:ROW_PAD]
        res_ref[ROW_PAD : 2 * ROW_PAD] = wide_ref[:ROW_PAD] + edge_ref[ROW_PAD:] * spill
        res_ref[2 * ROW_PAD :] = wide_ref[ROW_PAD:keep]

    @pl.when(core == 1)
    def _():
        spill = jnp.where(lat < n_lat - 1, 1.0, 0.0)
        res_ref[:keep] = wide_ref[:keep]
        res_ref[keep:] = edge_ref[:ROW_PAD] + wide_ref[keep:] * spill

    ocean = jnp.where(widened(0) > 0.0, 1.0, 0.0)
    res_ref[...] = res_ref[...] * ocean

    def inner(value):
        return value[ROW_PAD:keep, COL_PAD : COL_PAD + cols]

    def fold(left, right):
        value = inner(left) * inner(right)
        out = value[:8]
        for start in range(8, rows, 8):
            out = out + value[start : start + 8]
        lanes = out[:, :COL_PAD]
        for start in range(COL_PAD, cols, COL_PAD):
            lanes = lanes + out[:, start : start + COL_PAD]
        return jnp.sum(lanes, axis=(0, 1), keepdims=True)

    lane = lax.broadcasted_iota(jnp.int32, (1, COL_PAD), 1)

    def operate(source, target):
        field = source[...]
        target[...] = (
            diag_ref[...] * field
            - cn_ref[...] * moved(field, 0, False)
            - cs_ref[...] * moved(field, 0, True)
            - cw_ref[...] * moved(field, 1, False)
            - ce_ref[...] * moved(field, 1, True)
        )

    def reduced(values, turn):
        slot_ref[turn, pl.ds(me, 1)] = values[None]
        part_ref[turn] = values

        def post(k, carry):
            pltpu.make_async_remote_copy(
                src_ref=part_ref.at[turn],
                dst_ref=slot_ref.at[turn, me],
                send_sem=sum_send.at[turn],
                recv_sem=sum_recv.at[turn],
                device_id=place(lax.rem(me + k, total)),
                device_id_type=MESH,
            ).start()
            return carry

        lax.fori_loop(1, total, post, 0)
        block = slot_ref.at[turn, pl.ds(0, total - 1)]
        pltpu.make_async_copy(block, block, sum_recv.at[turn]).wait()
        pltpu.make_async_copy(block, block, sum_send.at[turn]).wait()
        return jnp.sum(slot_ref[turn], axis=0)

    def axpy(base, factor, extra):
        out = []
        for one, two in zip(base, extra):
            if two is None:
                out.append(one)
            else:
                out.append(factor * two if one is None else one + factor * two)
        return out

    unit = jnp.ones((1, 1), jnp.float32)
    dir_ref[...] = res_ref[...]
    done = 0
    for turn, count in enumerate(STAGES):
        along = [dir_ref, adir_ref, far_ref][: count + 1]
        across = [] if turn == 0 else [res_ref, app_ref][:count]
        for chain in (along, across):
            for source, target in zip(chain[:-1], chain[1:]):
                operate(source, target)
        vectors = along + across
        size = len(vectors)
        fields = [ref[...] for ref in vectors]
        pairs = [(i, j) for i in range(size) for j in range(i, size)]
        values = jnp.zeros((1, COL_PAD), jnp.float32)
        for number, (i, j) in enumerate(pairs):
            values = jnp.where(lane == number, fold(fields[i], fields[j]), values)
        sums = reduced(values, turn)
        gram = {}
        for number, (i, j) in enumerate(pairs):
            gram[i, j] = gram[j, i] = sums[:, number : number + 1]

        def quad(first, second):
            out = None
            for i in range(size):
                row = None
                for j in range(size):
                    if second[j] is not None:
                        term = second[j] * gram[i, j]
                        row = term if row is None else row + term
                if first[i] is not None:
                    out = first[i] * row if out is None else out + first[i] * row
            return out

        direct = [unit] + [None] * (size - 1)
        resid = [None] * size
        resid[count + 1 if across else 0] = unit
        gained = [None] * size
        norm = quad(resid, resid)
        for _ in range(count):
            done += 1
            applied = [None] + direct[:count]
            if across:
                applied += [None] + direct[count + 1 : size - 1]
            step_size = norm / quad(direct, applied)
            gained = axpy(gained, step_size, direct)
            resid = axpy(resid, -step_size, applied)
            if done < ITERS:
                norm_next = quad(resid, resid)
                direct = axpy(resid, norm_next / norm, direct)
                norm = norm_next

        def mix(weights, parts):
            out = None
            for weight, part in zip(weights, parts):
                if weight is not None:
                    out = weight * part if out is None else out + weight * part
            return out

        gain = mix(gained, [inner(field) for field in fields])
        sol_ref[...] = gain if turn == 0 else sol_ref[...] + gain
        res_ref[...] = mix(resid, fields)
        if done < ITERS:
            dir_ref[...] = mix(direct, fields)
    x_ref[...] = sol_ref[...]
    r_ref[...] = inner(res_ref[...])


def body(
    innovation, obs_error, obs_offset, obs_cell, obs_owner, block_count,
    land_mask, inertia, sea_depth,
):
    block_total = obs_owner.shape[1]
    block_width = innovation.shape[1]
    n_lat, n_lon, n_obs = (lax.axis_size(name) for name in AXES)
    tile_count = n_lat * n_lon
    capacity = max(3, 2 * ((block_total + tile_count - 1) // tile_count))
    rows, cols = land_mask.shape
    tile_rows = rows * n_obs
    half = cols // 2
    row_span = tile_rows + 8
    total = tile_count * n_obs
    owners = obs_owner[0]
    block_ids = jnp.arange(block_total)
    is_live = block_ids < block_count[0]
    earlier = block_ids[None, :] < block_ids[:, None]
    same_owner = (owners[None, :] == owners[:, None]) & earlier & is_live[None, :]
    slot_rank = jnp.sum(same_owner.astype(jnp.int32), axis=1)
    target = jnp.where(is_live, owners * capacity + slot_rank, tile_count * capacity)
    place = (jnp.arange(tile_count * capacity)[:, None] == target[None, :]).astype(jnp.float32)
    scaled = innovation / (obs_error * obs_error)
    cell_row, cell_col = obs_cell // cols, obs_cell % cols
    key = ((cell_col // half) * row_span + cell_row) * half + cell_col % half
    data = jnp.stack([scaled, obs_offset[0], obs_offset[1], key.astype(jnp.float32)], axis=1)
    sent = jnp.dot(
        place,
        data.reshape(block_total, 4 * block_width),
        precision=lax.Precision.HIGHEST,
        preferred_element_type=jnp.float32,
    )
    sent = sent.reshape(tile_count, capacity, 4, block_width).transpose(0, 2, 1, 3)
    tile = pl.pallas_call(
        functools.partial(spread_kernel, row_span, half),
        in_specs=[pl.BlockSpec(memory_space=pltpu.VMEM)],
        out_specs=pl.BlockSpec(memory_space=pltpu.VMEM),
        out_shape=jax.ShapeDtypeStruct((row_span, cols + COL_PAD), jnp.float32),
        scratch_shapes=[
            pltpu.VMEM((tile_count, 4, capacity, block_width), jnp.float32),
            pltpu.VMEM((8 * row_span, half), jnp.float32),
            pltpu.SemaphoreType.DMA((tile_count,)),
            pltpu.SemaphoreType.DMA((tile_count,)),
        ],
        compiler_params=pltpu.CompilerParams(collective_id=1, has_side_effects=True),
        name="spread",
    )(sent)
    conduct = land_mask.astype(jnp.float32) * sea_depth
    ground = jnp.stack([conduct, inertia])
    tall, broad = rows + 2 * ROW_PAD, cols + 2 * COL_PAD
    vmem = lambda *shape: pltpu.VMEM(shape, jnp.float32)
    return pl.pallas_call(
        solve_kernel,
        out_shape=[jax.ShapeDtypeStruct((rows, cols), jnp.float32)] * 2,
        in_specs=[pl.BlockSpec(memory_space=pltpu.VMEM)] * 2,
        out_specs=[pl.BlockSpec(memory_space=pltpu.VMEM)] * 2,
        scratch_shapes=[
            vmem(tall, cols + COL_PAD),
            vmem(tall, cols + COL_PAD),
            vmem(tall, 2 * COL_PAD),
            vmem(tall, COL_PAD),
            vmem(2 * ROW_PAD, broad),
            vmem(tall, broad),
            vmem(2, ROW_PAD, cols),
            vmem(2, ROW_PAD, cols),
            vmem(2, tall, cols),
            vmem(2, tall, COL_PAD),
            vmem(2, tall, COL_PAD),
        ]
        + [vmem(tall, broad)] * 10
        + [
            vmem(rows, cols),
            vmem(len(STAGES), 1, COL_PAD),
            vmem(len(STAGES), total, 1, COL_PAD),
            pltpu.SemaphoreType.DMA((8,)),
            pltpu.SemaphoreType.DMA((8,)),
            pltpu.SemaphoreType.DMA((len(STAGES),)),
            pltpu.SemaphoreType.DMA((len(STAGES),)),
        ],
        compiler_params=pltpu.CompilerParams(collective_id=0, has_side_effects=True),
        name="solve",
    )(tile, ground)


def solution(mesh):
    spread = P(AXES, None)
    grid = P(("lat", "obs"), "lon")
    in_specs = (spread, spread, P(None, AXES, None), spread, spread, P(AXES), grid, grid, grid)
    return jax.shard_map(
        body, mesh=mesh, in_specs=in_specs, out_specs=(grid, grid), check_vma=False
    )
```
